32 devices in a mesh: wide: 2 (over x), narrow: 4 (over y, core), depth: 4 (over z).
Axes of the slice: x: 2, y: 2, z: 4, core: 2. Of those that a mesh axis runs over, the one named last changes fastest.
Arguments:
- patch_store: bfloat16 [8, 1024, 4096], P('wide', 'depth'), may hold values from -6 to 6
- w_key: bfloat16 [4096, 1024], P(None, 'narrow'), may hold values from -0.09375 to 0.09375
- w_value: bfloat16 [4096, 1024], P(None, 'narrow'), may hold values from -0.09375 to 0.09375
- key_gain: float32 [128], replicated, may hold values from 0.1 to 1.9
- query_gain: float32 [128], replicated, may hold values from 0.1 to 1.9
- queries: bfloat16 [32, 4096], P('wide', 'narrow'), may hold values from -6 to 6
- owner_table: int32 [8], replicated, may hold values from 0 to 7, each once
- reader_table: int32 [2, 2], replicated, may hold values from 0 to 7
- request_image: int32 [32], P('wide'), may hold values from 0 to 1
- image_tiles: int32 [8], replicated, may hold values from 1 to 4
Outputs:
- context: bfloat16 [32, 4096], P(('wide', 'depth'), 'narrow')
The draws below stay inside these ranges and needn't reach their ends.
Inputs may be any that keep to these rules, and one draw needn't show every extreme that they name: owner_table is a permutation of the slots. `reader_table`: entries are image ids; a group's list may repeat an image.
All inputs are finite; a program needn't handle non-finite values.
Results may differ from the reference program's by a relative error of at most 0.012.
Values may be sent and summed in bfloat16 or wider, within the bound.
A program may use at most 64 MiB of HBM per device.

```python
import math
import jax
import jax.numpy as jnp
import numpy as np
from jax import lax

D = 4096
HEADS = 32
KV_HEADS = 8
HD = 128
TILES = 4
TILE_P = 256
READS = 2
PATCHES = 1024
IMAGES = 8
GROUPS = 2
BATCH = 32
N_WIDE = 2


def touch_ends(values, own_key, smallest, largest):
    place = [jax.random.randint(jax.random.fold_in(own_key, axis), (), 0, length) for axis, length in enumerate(values.shape)]
    main_axis = values.shape.index(max(values.shape))
    neighbour = place[:main_axis] + [(place[main_axis] + 1) % values.shape[main_axis]] + place[main_axis + 1:]
    return values.at[tuple(place)].set(smallest).at[tuple(neighbour)].set(largest)


def shard_levels(own_key, extent, split, smallest, high):
    def one(position, parts):
        heights = jax.random.uniform(jax.random.fold_in(jax.random.fold_in(own_key, 6), position), (parts,), jnp.float32, smallest / len(split), high / len(split))
        return jnp.repeat(jnp.exp(heights), extent[position] // parts).reshape((-1,) + (1,) * (len(extent) - position - 1))

    factor_of = one(*split[0])
    for cut in split[1:]:
        factor_of = factor_of * one(*cut)
    return factor_of


def rank_table(count, slope):
    portions = [(1 << 20) // math.isqrt(rank ** slope) + 1 for rank in range(1, count + 1)]
    spread = 1 + sum(portions) // (1 << 30)
    return np.cumsum(np.array([max(1, weight // spread) for weight in portions]))


def ranked_ids(key, extent, number_of, skew):
    table = rank_table(number_of, skew)
    lot = jax.random.randint(jax.random.fold_in(key, 1), extent, 0, int(table[number_of - 1]))
    standing = jnp.searchsorted(jnp.asarray(table, jnp.int32), lot, side="right")
    return jax.random.permutation(jax.random.fold_in(key, 2), number_of)[standing].astype(jnp.int32)


def centred(stream_key, shape, spread, reach, split=(), held_as=jnp.bfloat16):
    factor_of = shard_levels(stream_key, shape, split, -0.22, 0.18) if split else 1.0
    drawn = jax.random.normal(stream_key, shape, jnp.float32) * spread * factor_of
    return jnp.minimum(jnp.maximum(drawn, -reach), reach).astype(held_as)


def setup_inputs(seed: int = 0) -> dict:
    streams_of = jax.random.split(jax.random.key(seed), 11)
    return {
        "patch_store": centred(streams_of[0], (IMAGES, PATCHES, D), 1.0, 6.0, ((0, 2), (1, 4))),
        "w_key": centred(streams_of[1], (D, KV_HEADS * HD), D ** -0.5, 0.09375, ((1, 4),)),
        "w_value": centred(streams_of[2], (D, KV_HEADS * HD), D ** -0.5, 0.09375, ((1, 4),)),
        "key_gain": jnp.clip(1.0 + 0.18 * jax.random.normal(streams_of[3], (HD,), jnp.float32), 0.1, 1.9),
        "query_gain": jnp.clip(1.0 + 0.18 * jax.random.normal(streams_of[4], (HD,), jnp.float32), 0.1, 1.9),
        "queries": centred(streams_of[5], (BATCH, HEADS * HD), 1.0, 6.0, ((0, 2), (1, 4))),
        "owner_table": jax.random.permutation(streams_of[6], IMAGES).astype(jnp.int32),
        "reader_table": touch_ends(ranked_ids(streams_of[7], (GROUPS, READS), IMAGES, 1), jax.random.fold_in(streams_of[7], 3), 0, IMAGES - 1).astype(jnp.int32),
        "request_image": touch_ends(jax.random.randint(streams_of[8], (BATCH,), 0, READS), jax.random.fold_in(streams_of[8], 1), 0, READS - 1).astype(jnp.int32),
        "image_tiles": touch_ends(jax.random.randint(streams_of[9], (IMAGES,), 1, TILES + 1), jax.random.fold_in(streams_of[9], 1), 1, TILES).astype(jnp.int32),
    }


epsilon = 1e-05

def rms_scaled(tensor, scaling):
    return tensor / jnp.sqrt(lax.optimization_barrier(jnp.mean(tensor * tensor, axis=-1, keepdims=True)) + epsilon) * scaling

def reference(patch_store, w_key, w_value, key_gain, query_gain, queries, owner_table, reader_table, request_image, image_tiles):
    batch = queries.shape[0]
    per_group = batch // N_WIDE
    group_size = HEADS // KV_HEADS
    scale = 1.0 / math.sqrt(HD)

    def one_group(group_index):
        images = reader_table[group_index]
        slots = owner_table[images]
        patch_rows = patch_store[slots].reshape(READS * PATCHES, D)
        raw_keys = jnp.dot(patch_rows, w_key, preferred_element_type=jnp.float32).reshape(READS, PATCHES, KV_HEADS, HD)
        image_keys = rms_scaled(raw_keys, key_gain).astype(jnp.bfloat16)
        image_values = jnp.dot(patch_rows, w_value, preferred_element_type=jnp.float32).astype(jnp.bfloat16)
        image_values = image_values.reshape(READS, PATCHES, KV_HEADS, HD)
        first_row = (group_index * per_group).astype(jnp.int32)
        rows_here = lax.dynamic_slice_in_dim(queries, first_row, per_group, 0).astype(jnp.float32)
        normed = rms_scaled(rows_here.reshape(per_group, KV_HEADS, group_size, HD), query_gain).astype(jnp.bfloat16)
        entries = lax.dynamic_slice_in_dim(request_image, first_row, per_group, 0)
        scores = jnp.einsum('bkgd,rskd->bkgrs', normed.astype(jnp.float32), image_keys.astype(jnp.float32)) * scale
        chosen = (entries[:, None] == jnp.arange(READS, dtype=jnp.int32)[None, :]).astype(jnp.float32)
        usable = (jnp.arange(PATCHES, dtype=jnp.int32)[None, :] // TILE_P < image_tiles[images][:, None]).astype(jnp.float32)
        weights = jnp.exp(scores) * chosen[:, None, None, :, None] * usable[None, None, None]
        denominator = lax.optimization_barrier(jnp.sum(weights, axis=(3, 4)))
        numerator = jnp.einsum('bkgrs,rskd->bkgd', weights.astype(jnp.bfloat16).astype(jnp.float32), image_values.astype(jnp.float32))
        return (numerator / denominator[..., None]).astype(jnp.bfloat16).reshape(per_group, HEADS * HD)
    result = lax.map(one_group, jnp.arange(N_WIDE, dtype=jnp.int32))
    return result.reshape(batch, HEADS * HD)
```

```python
import functools
import math

import jax
import jax.numpy as jnp
from jax import lax
from jax.experimental import pallas as pl
from jax.experimental.pallas import tpu as pltpu
from jax.sharding import PartitionSpec as P

HD = 128
TILE_P = 256
EPSILON = 1e-05
CHUNKS = 4
LAG = 3
MESH = pl.DeviceIdType.MESH


def kernel(
    n_wide,
    n_depth,
    store,
    w_key,
    w_value,
    key_gain,
    query_gain,
    queries,
    owner_table,
    reader_table,
    request_image,
    image_tiles,
    out,
    xbuf,
    wbuf,
    qraw,
    gains,
    qf,
    qs,
    qx,
    row_slot,
    row_limit,
    raw,
    acc,
    msg,
    got,
    res,
    w_sem,
    x0_sem,
    x_sem,
    q_sem,
    q_send,
    q_recv,
    m_send,
    m_recv,
):
    images, rows, width = xbuf.shape
    kv_local = wbuf.shape[0]
    batch = qraw.shape[0]
    group = qraw.shape[1] // (kv_local * HD)
    share = batch // n_depth
    block = share * group
    group_rows = n_depth * block
    peers = n_wide * n_depth
    total_rows = peers * block
    chunk = width // CHUNKS
    wide, depth = lax.axis_index("wide"), lax.axis_index("depth")
    me = wide * n_depth + depth

    def weight_copies(k, c):
        piece = pl.ds(c * chunk, chunk)
        return [
            pltpu.make_async_copy(
                source.at[piece, pl.ds(k * HD, HD)],
                wbuf.at[k, piece, pl.ds(part * HD, HD)],
                w_sem.at[k, c, part],
            )
            for part, source in enumerate((w_key, w_value))
        ]

    def first_copy(c):
        piece = pl.ds(c * chunk, chunk)
        return pltpu.make_async_copy(store.at[0, :, piece], xbuf.at[0, :, piece], x0_sem.at[c])

    def image_copy(j):
        return pltpu.make_async_copy(store.at[j], xbuf.at[j], x_sem.at[j])

    small = [
        pltpu.make_async_copy(queries, qraw, q_sem.at[0]),
        pltpu.make_async_copy(query_gain, gains.at[0], q_sem.at[1]),
        pltpu.make_async_copy(key_gain, gains.at[1], q_sem.at[2]),
    ]
    for c in range(CHUNKS):
        for copy in weight_copies(0, c):
            copy.start()
        first_copy(c).start()
        if c == 0:
            for copy in small:
                copy.start()
    for j in range(1, images):
        image_copy(j).start()
    for k in range(1, kv_local):
        for c in range(CHUNKS):
            for copy in weight_copies(k, c):
                copy.start()

    barrier = pltpu.get_barrier_semaphore()

    def peer(offset):
        index = lax.rem(me + offset, peers)
        return index, {"wide": index // n_depth, "depth": lax.rem(index, n_depth)}

    def greet(offset, carry):
        pl.semaphore_signal(barrier, inc=1, device_id=peer(offset)[1], device_id_type=MESH)
        return carry

    lax.fori_loop(1, peers, greet, 0, unroll=peers <= 8)

    for copy in small:
        copy.wait()
    gain = gains[0] * gains[1] * (1.0 / math.sqrt(HD))
    for h in range(kv_local * group):
        lanes = pl.ds(h * HD, HD)
        head = qraw[:, lanes].astype(jnp.float32)
        mean = jnp.mean(head * head, axis=-1, keepdims=True)
        qf[:, lanes] = head * lax.rsqrt(mean + EPSILON) * gain
    for k in range(kv_local):
        for t in range(n_depth):
            for g in range(group):
                qs[pl.ds(t * block + g * share, share), :] = qf[
                    pl.ds(t * share, share), pl.ds((k * group + g) * HD, HD)
                ]
        qx[wide, k] = qs[...].astype(jnp.bfloat16)
    row = lax.broadcasted_iota(jnp.int32, (group_rows, HD), 0)
    request = row // block * share + row % share
    entry = jnp.zeros((group_rows, HD), jnp.int32)
    for b in range(batch):
        entry = jnp.where(request == b, request_image[b], entry)
    qx[wide, kv_local] = entry.astype(jnp.float32).astype(jnp.bfloat16)
    acc[...] = jnp.zeros_like(acc)

    def query_copy(offset):
        return pltpu.make_async_remote_copy(
            src_ref=qx.at[wide],
            dst_ref=qx.at[wide],
            send_sem=q_send.at[offset],
            recv_sem=q_recv.at[offset],
            device_id={"wide": lax.rem(wide + offset, n_wide)},
            device_id_type=MESH,
        )

    def query_landed(offset):
        source = lax.rem(wide + n_wide - offset, n_wide)
        return pltpu.make_async_remote_copy(
            src_ref=qx.at[source],
            dst_ref=qx.at[source],
            send_sem=q_send.at[offset],
            recv_sem=q_recv.at[offset],
            device_id={"wide": lax.rem(wide + offset, n_wide)},
            device_id_type=MESH,
        )

    def result_copy(k, offset):
        index, device = peer(offset)
        return pltpu.make_async_remote_copy(
            src_ref=msg.at[k, index],
            dst_ref=got.at[k, offset],
            send_sem=m_send.at[k, offset],
            recv_sem=m_recv.at[k, offset],
            device_id=device,
            device_id_type=MESH,
        )

    def send_results(k):
        def step(offset, carry):
            result_copy(k, offset).start()
            return carry

        lax.fori_loop(1, peers, step, 0, unroll=peers <= 8)

    whole_tiles = TILE_P % rows == 0

    def read_queries():
        for offset in range(1, n_wide):
            query_landed(offset).wait_recv()
        for g in range(n_wide):
            entry = qx[g, kv_local].astype(jnp.float32)
            slots = jnp.full((group_rows, HD), -1, jnp.int32)
            limits = jnp.zeros((group_rows, HD), jnp.int32)
            for r in range(reader_table.shape[1]):
                image = reader_table[g, r]
                slot = owner_table[image]
                limit = image_tiles[image] * TILE_P - depth * rows
                if whole_tiles:
                    slot = jnp.where(limit > 0, slot, -1)
                slots = jnp.where(entry == r, slot, slots)
                limits = jnp.where(entry == r, limit, limits)
            row_slot[pl.ds(g * group_rows, group_rows), :] = slots
            row_limit[pl.ds(g * group_rows, group_rows), :] = limits

    def wider(tile):
        return jnp.concatenate([tile] * (rows // HD), axis=1) if rows > HD else tile

    def attend(unit):
        k, j = divmod(unit, images)
        keys = raw[unit, :, :HD]
        mean = jnp.mean(keys * keys, axis=-1, keepdims=True)
        keys = (keys * lax.rsqrt(mean + EPSILON)).astype(jnp.bfloat16)
        values = raw[unit, :, HD:].astype(jnp.bfloat16)
        values = jnp.concatenate([values, jnp.ones_like(values)], axis=1)
        asked = qx[:, k].reshape(total_rows, HD)
        scores = lax.dot_general(
            asked, keys, (((1,), (1,)), ((), ())), preferred_element_type=jnp.float32
        )
        keep = wider(row_slot[...]) == wide * images + j
        if not whole_tiles:
            place = lax.broadcasted_iota(jnp.int32, (total_rows, rows), 1)
            keep = keep & (place < wider(row_limit[...]))
        weights = jnp.where(keep, jnp.exp(scores), 0.0).astype(jnp.bfloat16)
        acc[k] += jnp.dot(weights, values, preferred_element_type=jnp.float32)
        if j == images - 1:
            msg[k] = acc[k].astype(jnp.bfloat16).reshape(peers, block, 2 * HD)

    def project(unit):
        k, j = divmod(unit, images)
        if unit == 0:
            total = jnp.zeros((rows, 2 * HD), jnp.float32)
            for c in range(CHUNKS):
                for copy in weight_copies(0, c):
                    copy.wait()
                first_copy(c).wait()
                piece = pl.ds(c * chunk, chunk)
                total = total + jnp.dot(
                    xbuf[0, :, piece], wbuf[0, piece, :], preferred_element_type=jnp.float32
                )
            raw[unit] = total
            return
        if k == 0:
            image_copy(j).wait()
        elif j == 0:
            for c in range(CHUNKS):
                for copy in weight_copies(k, c):
                    copy.wait()
        raw[unit] = jnp.dot(xbuf[j], wbuf[k], preferred_element_type=jnp.float32)

    units = kv_local * images
    pending, sent, ready = [], 0, []
    for unit in range(units):
        project(unit)
        if unit == 0:
            pl.semaphore_wait(barrier, peers - 1)
            for offset in range(1, n_wide):
                query_copy(offset).start()
        for k in ready:
            send_results(k)
        ready = []
        if unit == min(LAG, units - 1):
            read_queries()
        if unit >= LAG:
            for old in pending[:2]:
                attend(old)
                if old % images == images - 1:
                    ready.append(old // images)
            pending = pending[2:]
        pending.append(unit)
    for old in pending:
        attend(old)
        if old % images == images - 1:
            ready.append(old // images)
    for k in ready:
        send_results(k)

    for k in range(kv_local):
        total = msg[k, me].astype(jnp.float32)

        def collect(offset, total, k=k):
            result_copy(k, offset).wait_recv()
            return total + got[k, offset].astype(jnp.float32)

        total = lax.fori_loop(1, peers, collect, total, unroll=peers <= 8)
        res[...] = total[:, :HD] / total[:, HD:]
        for g in range(group):
            out[:, pl.ds((k * group + g) * HD, HD)] = res[pl.ds(g * share, share), :].astype(
                out.dtype
            )

    for offset in range(1, n_wide):
        query_copy(offset).wait_send()
    for k in range(kv_local):

        def drain(offset, carry, k=k):
            result_copy(k, offset).wait_send()
            return carry

        lax.fori_loop(1, peers, drain, 0, unroll=peers <= 8)


def local(
    n_wide,
    n_depth,
    patch_store,
    w_key,
    w_value,
    key_gain,
    query_gain,
    queries,
    owner_table,
    reader_table,
    request_image,
    image_tiles,
):
    images, rows, width = patch_store.shape
    kv_local = w_key.shape[1] // HD
    batch, q_cols = queries.shape
    group = q_cols // (kv_local * HD)
    share = batch // n_depth
    block = share * group
    group_rows = n_depth * block
    peers = n_wide * n_depth
    total_rows = peers * block
    anywhere = pl.BlockSpec(memory_space=pl.ANY)
    scalars = pl.BlockSpec(memory_space=pltpu.SMEM)
    dma = pltpu.SemaphoreType.DMA
    return pl.pallas_call(
        functools.partial(kernel, n_wide, n_depth),
        out_shape=jax.ShapeDtypeStruct((share, q_cols), jnp.bfloat16),
        in_specs=[anywhere] * 6 + [scalars] * 4,
        out_specs=pl.BlockSpec(memory_space=pltpu.VMEM),
        scratch_shapes=[
            pltpu.VMEM((images, rows, width), jnp.bfloat16),
            pltpu.VMEM((kv_local, width, 2 * HD), jnp.bfloat16),
            pltpu.VMEM((batch, q_cols), jnp.bfloat16),
            pltpu.VMEM((2, 1, HD), jnp.float32),
            pltpu.VMEM((batch, q_cols), jnp.float32),
            pltpu.VMEM((group_rows, HD), jnp.float32),
            pltpu.VMEM((n_wide, kv_local + 1, group_rows, HD), jnp.bfloat16),
            pltpu.VMEM((total_rows, HD), jnp.int32),
            pltpu.VMEM((total_rows, HD), jnp.int32),
            pltpu.VMEM((kv_local * images, rows, 2 * HD), jnp.float32),
            pltpu.VMEM((kv_local, total_rows, 2 * HD), jnp.float32),
            pltpu.VMEM((kv_local, peers, block, 2 * HD), jnp.bfloat16),
            pltpu.VMEM((kv_local, peers, block, 2 * HD), jnp.bfloat16),
            pltpu.VMEM((block, HD), jnp.float32),
            dma((kv_local, CHUNKS, 2)),
            dma((CHUNKS,)),
            dma((images,)),
            dma((3,)),
            dma((n_wide,)),
            dma((n_wide,)),
            dma((kv_local, peers)),
            dma((kv_local, peers)),
        ],
        compiler_params=pltpu.CompilerParams(
            collective_id=0, has_side_effects=True, vmem_limit_bytes=56 * 1024 * 1024
        ),
    )(
        patch_store,
        w_key,
        w_value,
        key_gain.reshape(1, HD),
        query_gain.reshape(1, HD),
        queries,
        owner_table,
        reader_table,
        request_image,
        image_tiles,
    )


def solution(mesh):
    placed = (
        P("wide", "depth", None),
        P(None, "narrow"),
        P(None, "narrow"),
        P(),
        P(),
        P("wide", "narrow"),
        P(),
        P(),
        P("wide"),
        P(),
    )
    return jax.shard_map(
        functools.partial(local, mesh.shape["wide"], mesh.shape["depth"]),
        mesh=mesh,
        in_specs=placed,
        out_specs=P(("wide", "depth"), "narrow"),
        check_vma=False,
    )
```

```python
import functools
import math

import jax
import jax.numpy as jnp
from jax import lax
from jax.experimental import pallas as pl
from jax.experimental.pallas import tpu as pltpu
from jax.sharding import PartitionSpec as P

HD = 128
TILE_P = 256
EPSILON = 1e-05
CHUNKS = 4
MEET = 2
MESH = pl.DeviceIdType.MESH


def kernel(
    n_wide,
    n_depth,
    store,
    w_key,
    w_value,
    key_gain,
    query_gain,
    queries,
    owner_hbm,
    reader_hbm,
    request_hbm,
    tiles_hbm,
    out,
    owner_table,
    reader_table,
    request_image,
    image_tiles,
    xbuf,
    wbuf,
    qraw,
    gains,
    qf,
    qs,
    qx,
    row_slot,
    row_limit,
    raw,
    keys,
    values,
    msg,
    got,
    res,
    w_sem,
    x0_sem,
    x_sem,
    q_sem,
    q_send,
    q_recv,
    m_send,
    m_recv,
):
    images, rows, width = xbuf.shape
    kv_local = wbuf.shape[0]
    batch = qraw.shape[0]
    group = qraw.shape[1] // (kv_local * HD)
    share = batch // n_depth
    block = share * group
    group_rows = n_depth * block
    peers = n_wide * n_depth
    total_rows = peers * block
    chunk = width // CHUNKS
    wide, depth = lax.axis_index("wide"), lax.axis_index("depth")
    me = wide * n_depth + depth

    barrier = pltpu.get_barrier_semaphore()

    def peer(offset):
        there = {
            "wide": lax.rem(wide + offset // n_depth, n_wide),
            "depth": lax.rem(depth + offset % n_depth, n_depth),
        }
        return there["wide"] * n_depth + there["depth"], there

    def greet(offset, carry):
        pl.semaphore_signal(barrier, inc=1, device_id=peer(offset)[1], device_id_type=MESH)
        return carry

    lax.fori_loop(1, peers, greet, 0, unroll=peers <= 8)

    def weight_copies(k, c):
        piece = pl.ds(c * chunk, chunk)
        return [
            pltpu.make_async_copy(
                source.at[piece, pl.ds(k * HD, HD)],
                wbuf.at[k, piece, pl.ds(part * HD, HD)],
                w_sem.at[k, c, part],
            )
            for part, source in enumerate((w_key, w_value))
        ]

    def first_copy(c):
        piece = pl.ds(c * chunk, chunk)
        return pltpu.make_async_copy(store.at[0, :, piece], xbuf.at[0, :, piece], x0_sem.at[c])

    def image_copy(j):
        return pltpu.make_async_copy(store.at[j], xbuf.at[j], x_sem.at[j])

    small = [
        pltpu.make_async_copy(queries, qraw, q_sem.at[0]),
        pltpu.make_async_copy(query_gain, gains.at[0], q_sem.at[1]),
        pltpu.make_async_copy(key_gain, gains.at[1], q_sem.at[2]),
        pltpu.make_async_copy(owner_hbm, owner_table, q_sem.at[3]),
        pltpu.make_async_copy(reader_hbm, reader_table, q_sem.at[4]),
        pltpu.make_async_copy(request_hbm, request_image, q_sem.at[5]),
        pltpu.make_async_copy(tiles_hbm, image_tiles, q_sem.at[6]),
    ]
    for c in range(CHUNKS):
        for copy in weight_copies(0, c):
            copy.start()
        first_copy(c).start()
        if c == 0:
            for copy in small:
                copy.start()
    for j in range(1, images):
        image_copy(j).start()
    for k in range(1, kv_local):
        for c in range(CHUNKS):
            for copy in weight_copies(k, c):
                copy.start()

    for copy in small:
        copy.wait()
    gain = gains[0] * gains[1] * (1.0 / math.sqrt(HD))
    for h in range(kv_local * group):
        lanes = pl.ds(h * HD, HD)
        head = qraw[:, lanes].astype(jnp.float32)
        mean = jnp.mean(head * head, axis=-1, keepdims=True)
        qf[:, lanes] = head * lax.rsqrt(mean + EPSILON) * gain
    for k in range(kv_local):
        for t in range(n_depth):
            for g in range(group):
                qs[pl.ds(t * block + g * share, share), :] = qf[
                    pl.ds(t * share, share), pl.ds((k * group + g) * HD, HD)
                ]
        qx[wide, k] = qs[...].astype(jnp.bfloat16)
    row = lax.broadcasted_iota(jnp.int32, (group_rows, HD), 0)
    request = row // block * share + row % share
    entry = jnp.zeros((group_rows, HD), jnp.int32)
    for b in range(batch):
        entry = jnp.where(request == b, request_image[b], entry)
    qx[wide, kv_local] = entry.astype(jnp.float32).astype(jnp.bfloat16)

    def query_copy(offset):
        return pltpu.make_async_remote_copy(
            src_ref=qx.at[wide],
            dst_ref=qx.at[wide],
            send_sem=q_send.at[offset],
            recv_sem=q_recv.at[offset],
            device_id={"wide": lax.rem(wide + offset, n_wide)},
            device_id_type=MESH,
        )

    def query_landed(offset):
        source = lax.rem(wide + n_wide - offset, n_wide)
        return pltpu.make_async_remote_copy(
            src_ref=qx.at[source],
            dst_ref=qx.at[source],
            send_sem=q_send.at[offset],
            recv_sem=q_recv.at[offset],
            device_id={"wide": lax.rem(wide + offset, n_wide)},
            device_id_type=MESH,
        )

    def result_copy(k, offset):
        index, device = peer(offset)
        return pltpu.make_async_remote_copy(
            src_ref=msg.at[k, index],
            dst_ref=got.at[k, offset],
            send_sem=m_send.at[k, offset],
            recv_sem=m_recv.at[k, offset],
            device_id=device,
            device_id_type=MESH,
        )

    def send_results(k):
        def step(offset, carry):
            result_copy(k, offset).start()
            return carry

        lax.fori_loop(1, peers, step, 0, unroll=peers <= 8)

    whole_tiles = TILE_P % rows == 0

    def read_queries():
        for offset in range(1, n_wide):
            query_landed(offset).wait_recv()
        for g in range(n_wide):
            entry = qx[g, kv_local].astype(jnp.float32)
            slots = jnp.full((group_rows, HD), -1, jnp.int32)
            limits = jnp.zeros((group_rows, HD), jnp.int32)
            for r in range(reader_table.shape[1]):
                image = reader_table[g, r]
                slot = owner_table[image]
                limit = image_tiles[image] * TILE_P - depth * rows
                if whole_tiles:
                    slot = jnp.where(limit > 0, slot, -1)
                slots = jnp.where(entry == r, slot, slots)
                limits = jnp.where(entry == r, limit, limits)
            row_slot[pl.ds(g * group_rows, group_rows), :] = slots
            row_limit[pl.ds(g * group_rows, group_rows), :] = limits

    def wider(tile):
        return jnp.concatenate([tile] * (rows // HD), axis=1) if rows > HD else tile

    def prepare(unit):
        k, j = divmod(unit, images)
        span = pl.ds(j * rows, rows)
        total = raw[unit]
        head = total[:, :HD]
        mean = jnp.mean(head * head, axis=-1, keepdims=True)
        keys[k, span, :] = (head * lax.rsqrt(mean + EPSILON)).astype(jnp.bfloat16)
        value = total[:, HD:].astype(jnp.bfloat16)
        values[k, span, :] = jnp.concatenate([value, jnp.ones_like(value)], axis=1)

    def attend_groups(k, start, count):
        span = pl.ds(start * group_rows, count * group_rows)
        asked = qx[pl.ds(start, count), k].reshape(count * group_rows, HD)
        wanted, limits = wider(row_slot[span, :]), wider(row_limit[span, :])
        scores = lax.dot_general(
            asked, keys[k], (((1,), (1,)), ((), ())), preferred_element_type=jnp.float32
        )
        weights = []
        for j in range(images):
            keep = wanted == wide * images + j
            if not whole_tiles:
                place = lax.broadcasted_iota(jnp.int32, keep.shape, 1)
                keep = keep & (place < limits)
            part = jnp.exp(scores[:, j * rows : (j + 1) * rows])
            weights.append(jnp.where(keep, part, 0.0).astype(jnp.bfloat16))
        total = jnp.dot(
            jnp.concatenate(weights, axis=1), values[k], preferred_element_type=jnp.float32
        )
        msg[k, pl.ds(start * n_depth, count * n_depth)] = total.astype(jnp.bfloat16).reshape(
            count * n_depth, block, 2 * HD
        )

    def attend(k):
        if n_wide <= 2:
            attend_groups(k, 0, n_wide)
        else:

            def step(g, carry):
                attend_groups(k, g, 1)
                return carry

            lax.fori_loop(0, n_wide, step, 0)

    def project(unit):
        k, j = divmod(unit, images)
        if unit == 0:
            total = jnp.zeros((rows, 2 * HD), jnp.float32)
            for c in range(CHUNKS):
                for copy in weight_copies(0, c):
                    copy.wait()
                first_copy(c).wait()
                piece = pl.ds(c * chunk, chunk)
                total = total + jnp.dot(
                    xbuf[0, :, piece], wbuf[0, piece, :], preferred_element_type=jnp.float32
                )
            raw[unit] = total
            return
        if k == 0:
            image_copy(j).wait()
        elif j == 0:
            for c in range(CHUNKS):
                for copy in weight_copies(k, c):
                    copy.wait()
        raw[unit] = jnp.dot(xbuf[j], wbuf[k], preferred_element_type=jnp.float32)

    units = kv_local * images
    meet = min(MEET, units - 1)
    for unit in range(units):
        project(unit)
        if unit > 0:
            prepare(unit - 1)
        if unit == meet:
            pl.semaphore_wait(barrier, peers - 1)
            for offset in range(1, n_wide):
                query_copy(offset).start()
    prepare(units - 1)
    read_queries()
    for k in range(kv_local):
        attend(k)
        send_results(k)

    for k in range(kv_local):
        total = msg[k, me].astype(jnp.float32)

        def collect(offset, total, k=k):
            result_copy(k, offset).wait_recv()
            return total + got[k, offset].astype(jnp.float32)

        total = lax.fori_loop(1, peers, collect, total, unroll=peers <= 8)
        res[...] = total[:, :HD] / total[:, HD:]
        for g in range(group):
            out[:, pl.ds((k * group + g) * HD, HD)] = res[pl.ds(g * share, share), :].astype(
                out.dtype
            )

    for offset in range(1, n_wide):
        query_copy(offset).wait_send()
    for k in range(kv_local):

        def drain(offset, carry, k=k):
            result_copy(k, offset).wait_send()
            return carry

        lax.fori_loop(1, peers, drain, 0, unroll=peers <= 8)


def local(
    n_wide,
    n_depth,
    patch_store,
    w_key,
    w_value,
    key_gain,
    query_gain,
    queries,
    owner_table,
    reader_table,
    request_image,
    image_tiles,
):
    images, rows, width = patch_store.shape
    kv_local = w_key.shape[1] // HD
    batch, q_cols = queries.shape
    group = q_cols // (kv_local * HD)
    share = batch // n_depth
    block = share * group
    group_rows = n_depth * block
    peers = n_wide * n_depth
    total_rows = peers * block
    anywhere = pl.BlockSpec(memory_space=pl.ANY)
    dma = pltpu.SemaphoreType.DMA
    return pl.pallas_call(
        functools.partial(kernel, n_wide, n_depth),
        out_shape=jax.ShapeDtypeStruct((share, q_cols), jnp.bfloat16),
        in_specs=[anywhere] * 10,
        out_specs=pl.BlockSpec(memory_space=pltpu.VMEM),
        scratch_shapes=[
            pltpu.SMEM(owner_table.shape, jnp.int32),
            pltpu.SMEM(reader_table.shape, jnp.int32),
            pltpu.SMEM(request_image.shape, jnp.int32),
            pltpu.SMEM(image_tiles.shape, jnp.int32),
            pltpu.VMEM((images, rows, width), jnp.bfloat16),
            pltpu.VMEM((kv_local, width, 2 * HD), jnp.bfloat16),
            pltpu.VMEM((batch, q_cols), jnp.bfloat16),
            pltpu.VMEM((2, 1, HD), jnp.float32),
            pltpu.VMEM((batch, q_cols), jnp.float32),
            pltpu.VMEM((group_rows, HD), jnp.float32),
            pltpu.VMEM((n_wide, kv_local + 1, group_rows, HD), jnp.bfloat16),
            pltpu.VMEM((total_rows, HD), jnp.int32),
            pltpu.VMEM((total_rows, HD), jnp.int32),
            pltpu.VMEM((kv_local * images, rows, 2 * HD), jnp.float32),
            pltpu.VMEM((kv_local, images * rows, HD), jnp.bfloat16),
            pltpu.VMEM((kv_local, images * rows, 2 * HD), jnp.bfloat16),
            pltpu.VMEM((kv_local, peers, block, 2 * HD), jnp.bfloat16),
            pltpu.VMEM((kv_local, peers, block, 2 * HD), jnp.bfloat16),
            pltpu.VMEM((block, HD), jnp.float32),
            dma((kv_local, CHUNKS, 2)),
            dma((CHUNKS,)),
            dma((images,)),
            dma((7,)),
            dma((n_wide,)),
            dma((n_wide,)),
            dma((kv_local, peers)),
            dma((kv_local, peers)),
        ],
        compiler_params=pltpu.CompilerParams(
            collective_id=0, has_side_effects=True, vmem_limit_bytes=56 * 1024 * 1024
        ),
    )(
        patch_store,
        w_key,
        w_value,
        key_gain.reshape(1, HD),
        query_gain.reshape(1, HD),
        queries,
        owner_table,
        reader_table,
        request_image,
        image_tiles,
    )


def solution(mesh):
    placed = (
        P("wide", "depth", None),
        P(None, "narrow"),
        P(None, "narrow"),
        P(),
        P(),
        P("wide", "narrow"),
        P(),
        P(),
        P("wide"),
        P(),
    )
    return jax.shard_map(
        functools.partial(local, mesh.shape["wide"], mesh.shape["depth"]),
        mesh=mesh,
        in_specs=placed,
        out_specs=P(("wide", "depth"), "narrow"),
        check_vma=False,
    )
```

```python
import functools
import math

import jax
import jax.numpy as jnp
from jax import lax
from jax.experimental import pallas as pl
from jax.experimental.pallas import tpu as pltpu
from jax.sharding import PartitionSpec as P

HD = 128
TILE_P = 256
EPSILON = 1e-05
CHUNKS = 4
MEET = 1
MESH = pl.DeviceIdType.MESH


def kernel(
    n_wide,
    n_depth,
    store,
    w_key,
    w_value,
    key_gain,
    query_gain,
    queries,
    owner_hbm,
    reader_hbm,
    request_hbm,
    tiles_hbm,
    out,
    owner_table,
    reader_table,
    request_image,
    image_tiles,
    xbuf,
    wbuf,
    qraw,
    gains,
    qf,
    qs,
    qx,
    row_slot,
    row_limit,
    raw,
    keys,
    values,
    msg,
    got,
    res,
    w_sem,
    x_sem,
    q_sem,
    q_send,
    q_recv,
    m_send,
    m_recv,
):
    images, rows, width = xbuf.shape
    kv_local = wbuf.shape[0]
    batch = qraw.shape[0]
    group = qraw.shape[1] // (kv_local * HD)
    share = batch // n_depth
    block = share * group
    group_rows = n_depth * block
    peers = n_wide * n_depth
    total_rows = peers * block
    chunk = width // CHUNKS
    wide, depth = lax.axis_index("wide"), lax.axis_index("depth")
    me = wide * n_depth + depth

    barrier = pltpu.get_barrier_semaphore()

    def peer(offset):
        there = {
            "wide": lax.rem(wide + offset // n_depth, n_wide),
            "depth": lax.rem(depth + offset % n_depth, n_depth),
        }
        return there["wide"] * n_depth + there["depth"], there

    def greet(offset, carry):
        pl.semaphore_signal(barrier, inc=1, device_id=peer(offset)[1], device_id_type=MESH)
        return carry

    lax.fori_loop(1, peers, greet, 0, unroll=peers <= 8)

    def weight_copies(k, c):
        piece = pl.ds(c * chunk, chunk)
        return [
            pltpu.make_async_copy(
                source.at[piece, pl.ds(k * HD, HD)],
                wbuf.at[k, piece, pl.ds(part * HD, HD)],
                w_sem.at[k, c, part],
            )
            for part, source in enumerate((w_key, w_value))
        ]

    def patch_copy(c):
        piece = pl.ds(c * chunk, chunk)
        return pltpu.make_async_copy(store.at[:, :, piece], xbuf.at[:, :, piece], x_sem.at[c])

    small = [
        pltpu.make_async_copy(queries, qraw, q_sem.at[0]),
        pltpu.make_async_copy(query_gain, gains.at[0], q_sem.at[1]),
        pltpu.make_async_copy(key_gain, gains.at[1], q_sem.at[2]),
        pltpu.make_async_copy(owner_hbm, owner_table, q_sem.at[3]),
        pltpu.make_async_copy(reader_hbm, reader_table, q_sem.at[4]),
        pltpu.make_async_copy(request_hbm, request_image, q_sem.at[5]),
        pltpu.make_async_copy(tiles_hbm, image_tiles, q_sem.at[6]),
    ]
    for c in range(CHUNKS):
        for k in range(kv_local):
            for copy in weight_copies(k, c):
                copy.start()
        patch_copy(c).start()
        if c == 0:
            for copy in small:
                copy.start()

    for copy in small:
        copy.wait()
    gain = gains[0] * gains[1] * (1.0 / math.sqrt(HD))
    for h in range(kv_local * group):
        lanes = pl.ds(h * HD, HD)
        head = qraw[:, lanes].astype(jnp.float32)
        mean = jnp.mean(head * head, axis=-1, keepdims=True)
        qf[:, lanes] = head * lax.rsqrt(mean + EPSILON) * gain
    for k in range(kv_local):
        for t in range(n_depth):
            for g in range(group):
                qs[pl.ds(t * block + g * share, share), :] = qf[
                    pl.ds(t * share, share), pl.ds((k * group + g) * HD, HD)
                ]
        qx[wide, k] = qs[...].astype(jnp.bfloat16)
    row = lax.broadcasted_iota(jnp.int32, (group_rows, HD), 0)
    request = row // block * share + row % share
    entry = jnp.zeros((group_rows, HD), jnp.int32)
    for b in range(batch):
        entry = jnp.where(request == b, request_image[b], entry)
    qx[wide, kv_local] = entry.astype(jnp.float32).astype(jnp.bfloat16)

    def query_copy(offset):
        return pltpu.make_async_remote_copy(
            src_ref=qx.at[wide],
            dst_ref=qx.at[wide],
            send_sem=q_send.at[offset],
            recv_sem=q_recv.at[offset],
            device_id={"wide": lax.rem(wide + offset, n_wide)},
            device_id_type=MESH,
        )

    def query_landed(offset):
        source = lax.rem(wide + n_wide - offset, n_wide)
        return pltpu.make_async_remote_copy(
            src_ref=qx.at[source],
            dst_ref=qx.at[source],
            send_sem=q_send.at[offset],
            recv_sem=q_recv.at[offset],
            device_id={"wide": lax.rem(wide + offset, n_wide)},
            device_id_type=MESH,
        )

    def result_copy(k, offset):
        index, device = peer(offset)
        return pltpu.make_async_remote_copy(
            src_ref=msg.at[k, index],
            dst_ref=got.at[k, offset],
            send_sem=m_send.at[k, offset],
            recv_sem=m_recv.at[k, offset],
            device_id=device,
            device_id_type=MESH,
        )

    def send_results(k):
        def step(offset, carry):
            result_copy(k, offset).start()
            return carry

        lax.fori_loop(1, peers, step, 0, unroll=peers <= 8)

    whole_tiles = TILE_P % rows == 0

    def read_queries():
        for offset in range(1, n_wide):
            query_landed(offset).wait_recv()
        for g in range(n_wide):
            entry = qx[g, kv_local].astype(jnp.float32)
            slots = jnp.full((group_rows, HD), -1, jnp.int32)
            limits = jnp.zeros((group_rows, HD), jnp.int32)
            for r in range(reader_table.shape[1]):
                image = reader_table[g, r]
                slot = owner_table[image]
                limit = image_tiles[image] * TILE_P - depth * rows
                if whole_tiles:
                    slot = jnp.where(limit > 0, slot, -1)
                slots = jnp.where(entry == r, slot, slots)
                limits = jnp.where(entry == r, limit, limits)
            row_slot[pl.ds(g * group_rows, group_rows), :] = slots
            row_limit[pl.ds(g * group_rows, group_rows), :] = limits

    def wider(tile):
        return jnp.concatenate([tile] * (rows // HD), axis=1) if rows > HD else tile

    def prepare(k):
        total = raw[k]
        head = total[:, :HD]
        mean = jnp.mean(head * head, axis=-1, keepdims=True)
        keys[k] = (head * lax.rsqrt(mean + EPSILON)).astype(jnp.bfloat16)
        value = total[:, HD:].astype(jnp.bfloat16)
        values[k] = jnp.concatenate([value, jnp.ones_like(value)], axis=1)

    def attend_groups(k, start, count):
        span = pl.ds(start * group_rows, count * group_rows)
        asked = qx[pl.ds(start, count), k].reshape(count * group_rows, HD)
        wanted, limits = wider(row_slot[span, :]), wider(row_limit[span, :])
        scores = lax.dot_general(
            asked, keys[k], (((1,), (1,)), ((), ())), preferred_element_type=jnp.float32
        )
        weights = []
        for j in range(images):
            keep = wanted == wide * images + j
            if not whole_tiles:
                place = lax.broadcasted_iota(jnp.int32, keep.shape, 1)
                keep = keep & (place < limits)
            part = jnp.exp(scores[:, j * rows : (j + 1) * rows])
            weights.append(jnp.where(keep, part, 0.0).astype(jnp.bfloat16))
        total = jnp.dot(
            jnp.concatenate(weights, axis=1), values[k], preferred_element_type=jnp.float32
        )
        msg[k, pl.ds(start * n_depth, count * n_depth)] = total.astype(jnp.bfloat16).reshape(
            count * n_depth, block, 2 * HD
        )

    def attend(k):
        if n_wide <= 2:
            attend_groups(k, 0, n_wide)
        else:

            def step(g, carry):
                attend_groups(k, g, 1)
                return carry

            lax.fori_loop(0, n_wide, step, 0)

    def project(k, c):
        piece = pl.ds(c * chunk, chunk)
        part = jnp.dot(
            xbuf[:, :, piece].reshape(images * rows, chunk),
            wbuf[k, piece, :],
            preferred_element_type=jnp.float32,
        )
        raw[k] = part if c == 0 else raw[k] + part

    for c in range(CHUNKS):
        for k in range(kv_local):
            for copy in weight_copies(k, c):
                copy.wait()
        patch_copy(c).wait()
        for k in range(kv_local):
            project(k, c)
            if c == CHUNKS - 1:
                prepare(k)
        if c == min(MEET, CHUNKS - 1):
            pl.semaphore_wait(barrier, peers - 1)
            for offset in range(1, n_wide):
                query_copy(offset).start()
    read_queries()
    for k in range(kv_local):
        attend(k)
        send_results(k)

    for k in range(kv_local):
        total = msg[k, me].astype(jnp.float32)

        def collect(offset, total, k=k):
            result_copy(k, offset).wait_recv()
            return total + got[k, offset].astype(jnp.float32)

        total = lax.fori_loop(1, peers, collect, total, unroll=peers <= 8)
        res[...] = total[:, :HD] / total[:, HD:]
        for g in range(group):
            out[:, pl.ds((k * group + g) * HD, HD)] = res[pl.ds(g * share, share), :].astype(
                out.dtype
            )

    for offset in range(1, n_wide):
        query_copy(offset).wait_send()
    for k in range(kv_local):

        def drain(offset, carry, k=k):
            result_copy(k, offset).wait_send()
            return carry

        lax.fori_loop(1, peers, drain, 0, unroll=peers <= 8)


def local(
    n_wide,
    n_depth,
    patch_store,
    w_key,
    w_value,
    key_gain,
    query_gain,
    queries,
    owner_table,
    reader_table,
    request_image,
    image_tiles,
):
    images, rows, width = patch_store.shape
    kv_local = w_key.shape[1] // HD
    batch, q_cols = queries.shape
    group = q_cols // (kv_local * HD)
    share = batch // n_depth
    block = share * group
    group_rows = n_depth * block
    peers = n_wide * n_depth
    total_rows = peers * block
    anywhere = pl.BlockSpec(memory_space=pl.ANY)
    dma = pltpu.SemaphoreType.DMA
    return pl.pallas_call(
        functools.partial(kernel, n_wide, n_depth),
        out_shape=jax.ShapeDtypeStruct((share, q_cols), jnp.bfloat16),
        in_specs=[anywhere] * 10,
        out_specs=pl.BlockSpec(memory_space=pltpu.VMEM),
        scratch_shapes=[
            pltpu.SMEM(owner_table.shape, jnp.int32),
            pltpu.SMEM(reader_table.shape, jnp.int32),
            pltpu.SMEM(request_image.shape, jnp.int32),
            pltpu.SMEM(image_tiles.shape, jnp.int32),
            pltpu.VMEM((images, rows, width), jnp.bfloat16),
            pltpu.VMEM((kv_local, width, 2 * HD), jnp.bfloat16),
            pltpu.VMEM((batch, q_cols), jnp.bfloat16),
            pltpu.VMEM((2, 1, HD), jnp.float32),
            pltpu.VMEM((batch, q_cols), jnp.float32),
            pltpu.VMEM((group_rows, HD), jnp.float32),
            pltpu.VMEM((n_wide, kv_local + 1, group_rows, HD), jnp.bfloat16),
            pltpu.VMEM((total_rows, HD), jnp.int32),
            pltpu.VMEM((total_rows, HD), jnp.int32),
            pltpu.VMEM((kv_local, images * rows, 2 * HD), jnp.float32),
            pltpu.VMEM((kv_local, images * rows, HD), jnp.bfloat16),
            pltpu.VMEM((kv_local, images * rows, 2 * HD), jnp.bfloat16),
            pltpu.VMEM((kv_local, peers, block, 2 * HD), jnp.bfloat16),
            pltpu.VMEM((kv_local, peers, block, 2 * HD), jnp.bfloat16),
            pltpu.VMEM((block, HD), jnp.float32),
            dma((kv_local, CHUNKS, 2)),
            dma((CHUNKS,)),
            dma((7,)),
            dma((n_wide,)),
            dma((n_wide,)),
            dma((kv_local, peers)),
            dma((kv_local, peers)),
        ],
        compiler_params=pltpu.CompilerParams(
            collective_id=0, has_side_effects=True, vmem_limit_bytes=56 * 1024 * 1024
        ),
    )(
        patch_store,
        w_key,
        w_value,
        key_gain.reshape(1, HD),
        query_gain.reshape(1, HD),
        queries,
        owner_table,
        reader_table,
        request_image,
        image_tiles,
    )


def solution(mesh):
    placed = (
        P("wide", "depth", None),
        P(None, "narrow"),
        P(None, "narrow"),
        P(),
        P(),
        P("wide", "narrow"),
        P(),
        P(),
        P("wide"),
        P(),
    )
    return jax.shard_map(
        functools.partial(local, mesh.shape["wide"], mesh.shape["depth"]),
        mesh=mesh,
        in_specs=placed,
        out_specs=P(("wide", "depth"), "narrow"),
        check_vma=False,
    )
```

```python
import functools
import math

import jax
import jax.numpy as jnp
from jax import lax
from jax.experimental import pallas as pl
from jax.experimental.pallas import tpu as pltpu
from jax.sharding import PartitionSpec as P

HD = 128
TILE_P = 256
EPSILON = 1e-05
CHUNKS = 4
MEET = 0
MESH = pl.DeviceIdType.MESH


def kernel(
    n_wide,
    n_depth,
    store,
    w_key,
    w_value,
    key_gain,
    query_gain,
    queries,
    owner_hbm,
    reader_hbm,
    request_hbm,
    tiles_hbm,
    out,
    owner_table,
    reader_table,
    request_image,
    image_tiles,
    xbuf,
    wbuf,
    qraw,
    gains,
    qf,
    qs,
    qx,
    row_slot,
    row_limit,
    raw,
    keys,
    values,
    msg,
    got,
    res,
    w_sem,
    x_sem,
    q_sem,
    q_send,
    q_recv,
    m_send,
    m_recv,
):
    images, rows, width = xbuf.shape
    kv_local = wbuf.shape[0]
    batch = qraw.shape[0]
    group = qraw.shape[1] // (kv_local * HD)
    share = batch // n_depth
    block = share * group
    group_rows = n_depth * block
    peers = n_wide * n_depth
    total_rows = peers * block
    chunk = width // CHUNKS
    wide, depth = lax.axis_index("wide"), lax.axis_index("depth")
    me = wide * n_depth + depth
    part_lanes = HD // kv_local

    barrier = pltpu.get_barrier_semaphore()

    def peer(offset):
        there = {
            "wide": lax.rem(wide + offset // n_depth, n_wide),
            "depth": lax.rem(depth + offset % n_depth, n_depth),
        }
        return there["wide"] * n_depth + there["depth"], there

    def greet(offset, carry):
        pl.semaphore_signal(barrier, inc=1, device_id=peer(offset)[1], device_id_type=MESH)
        return carry

    lax.fori_loop(1, peers, greet, 0, unroll=peers <= 8)

    def weight_copies(k, c):
        piece = pl.ds(c * chunk, chunk)
        return [
            pltpu.make_async_copy(
                source.at[piece, pl.ds(k * HD, HD)],
                wbuf.at[k, piece, pl.ds(part * HD, HD)],
                w_sem.at[k, c, part],
            )
            for part, source in enumerate((w_key, w_value))
        ]

    def patch_copy(c):
        piece = pl.ds(c * chunk, chunk)
        return pltpu.make_async_copy(store.at[:, :, piece], xbuf.at[:, :, piece], x_sem.at[c])

    small = [
        pltpu.make_async_copy(queries, qraw, q_sem.at[0]),
        pltpu.make_async_copy(query_gain, gains.at[0], q_sem.at[1]),
        pltpu.make_async_copy(key_gain, gains.at[1], q_sem.at[2]),
        pltpu.make_async_copy(owner_hbm, owner_table, q_sem.at[3]),
        pltpu.make_async_copy(reader_hbm, reader_table, q_sem.at[4]),
        pltpu.make_async_copy(request_hbm, request_image, q_sem.at[5]),
        pltpu.make_async_copy(tiles_hbm, image_tiles, q_sem.at[6]),
    ]
    for c in range(CHUNKS):
        for k in range(kv_local):
            for copy in weight_copies(k, c):
                copy.start()
        patch_copy(c).start()
        if c == 0:
            for copy in small:
                copy.start()

    for copy in small:
        copy.wait()
    gain = gains[0] * gains[1] * (1.0 / math.sqrt(HD))
    for h in range(kv_local * group):
        lanes = pl.ds(h * HD, HD)
        head = qraw[:, lanes].astype(jnp.float32)
        mean = jnp.mean(head * head, axis=-1, keepdims=True)
        qf[:, lanes] = head * lax.rsqrt(mean + EPSILON) * gain
    for k in range(kv_local):
        for t in range(n_depth):
            for g in range(group):
                qs[pl.ds(t * block + g * share, share), :] = qf[
                    pl.ds(t * share, share), pl.ds((k * group + g) * HD, HD)
                ]
        qx[wide, k] = qs[...].astype(jnp.bfloat16)
    row = lax.broadcasted_iota(jnp.int32, (group_rows, HD), 0)
    request = row // block * share + row % share
    entry = jnp.zeros((group_rows, HD), jnp.int32)
    for b in range(batch):
        entry = jnp.where(request == b, request_image[b], entry)
    qx[wide, kv_local] = entry.astype(jnp.float32).astype(jnp.bfloat16)

    def query_copy(offset):
        return pltpu.make_async_remote_copy(
            src_ref=qx.at[wide],
            dst_ref=qx.at[wide],
            send_sem=q_send.at[offset],
            recv_sem=q_recv.at[offset],
            device_id={"wide": lax.rem(wide + offset, n_wide)},
            device_id_type=MESH,
        )

    def query_landed(offset):
        source = lax.rem(wide + n_wide - offset, n_wide)
        return pltpu.make_async_remote_copy(
            src_ref=qx.at[source],
            dst_ref=qx.at[source],
            send_sem=q_send.at[offset],
            recv_sem=q_recv.at[offset],
            device_id={"wide": lax.rem(wide + offset, n_wide)},
            device_id_type=MESH,
        )

    def result_copy(offset):
        index, device = peer(offset)
        return pltpu.make_async_remote_copy(
            src_ref=msg.at[index],
            dst_ref=got.at[offset],
            send_sem=m_send.at[offset],
            recv_sem=m_recv.at[offset],
            device_id=device,
            device_id_type=MESH,
        )

    def send_results():
        def step(offset, carry):
            result_copy(offset).start()
            return carry

        lax.fori_loop(1, peers, step, 0, unroll=peers <= 8)

    whole_tiles = TILE_P % rows == 0

    def read_queries():
        for offset in range(1, n_wide):
            query_landed(offset).wait_recv()
        for g in range(n_wide):
            entry = qx[g, kv_local].astype(jnp.float32)
            slots = jnp.full((group_rows, HD), -1, jnp.int32)
            limits = jnp.zeros((group_rows, HD), jnp.int32)
            for r in range(reader_table.shape[1]):
                image = reader_table[g, r]
                slot = owner_table[image]
                limit = image_tiles[image] * TILE_P - depth * rows
                if whole_tiles:
                    slot = jnp.where(limit > 0, slot, -1)
                slots = jnp.where(entry == r, slot, slots)
                limits = jnp.where(entry == r, limit, limits)
            row_slot[pl.ds(g * group_rows, group_rows), :] = slots
            row_limit[pl.ds(g * group_rows, group_rows), :] = limits

    def wider(tile):
        return jnp.concatenate([tile] * (rows // HD), axis=1) if rows > HD else tile

    def prepare(k):
        total = raw[k]
        head = total[:, :HD]
        mean = jnp.mean(head * head, axis=-1, keepdims=True)
        keys[k] = (head * lax.rsqrt(mean + EPSILON)).astype(jnp.bfloat16)
        value = total[:, HD:].astype(jnp.bfloat16)
        values[k] = jnp.concatenate([value, jnp.ones_like(value)], axis=1)

    def attend_groups(k, start, count):
        span = pl.ds(start * group_rows, count * group_rows)
        asked = qx[pl.ds(start, count), k].reshape(count * group_rows, HD)
        wanted, limits = wider(row_slot[span, :]), wider(row_limit[span, :])
        scores = lax.dot_general(
            asked, keys[k], (((1,), (1,)), ((), ())), preferred_element_type=jnp.float32
        )
        weights = []
        for j in range(images):
            keep = wanted == wide * images + j
            if not whole_tiles:
                place = lax.broadcasted_iota(jnp.int32, keep.shape, 1)
                keep = keep & (place < limits)
            part = jnp.exp(scores[:, j * rows : (j + 1) * rows])
            weights.append(jnp.where(keep, part, 0.0).astype(jnp.bfloat16))
        total = jnp.dot(
            jnp.concatenate(weights, axis=1), values[k], preferred_element_type=jnp.float32
        )
        total = total.astype(jnp.bfloat16).reshape(count * n_depth, block, 2 * HD)
        dest = pl.ds(start * n_depth, count * n_depth)
        msg[dest, k] = total[:, :, :HD]
        below = total[:, :, HD:]
        if k:
            lane = lax.broadcasted_iota(jnp.int32, below.shape, 2)
            older = msg[dest, kv_local].astype(jnp.float32)
            below = jnp.where(lane < k * part_lanes, older, below.astype(jnp.float32))
        msg[dest, kv_local] = below.astype(jnp.bfloat16)

    def attend(k):
        if n_wide <= 2:
            attend_groups(k, 0, n_wide)
        else:

            def step(g, carry):
                attend_groups(k, g, 1)
                return carry

            lax.fori_loop(0, n_wide, step, 0)

    def project(k, c):
        piece = pl.ds(c * chunk, chunk)
        part = jnp.dot(
            xbuf[:, :, piece].reshape(images * rows, chunk),
            wbuf[k, piece, :],
            preferred_element_type=jnp.float32,
        )
        raw[k] = part if c == 0 else raw[k] + part

    for c in range(CHUNKS):
        for k in range(kv_local):
            for copy in weight_copies(k, c):
                copy.wait()
        patch_copy(c).wait()
        for k in range(kv_local):
            project(k, c)
            if c == CHUNKS - 1:
                prepare(k)
        if c == min(MEET, CHUNKS - 1):
            pl.semaphore_wait(barrier, peers - 1)
            for offset in range(1, n_wide):
                query_copy(offset).start()
    read_queries()
    for k in range(kv_local):
        attend(k)
    send_results()

    total = msg[me].astype(jnp.float32)

    def collect(offset, total):
        result_copy(offset).wait_recv()
        return total + got[offset].astype(jnp.float32)

    total = lax.fori_loop(1, peers, collect, total, unroll=peers <= 8)
    for k in range(kv_local):
        res[...] = total[k] / total[kv_local, :, k * part_lanes : k * part_lanes + 1]
        for g in range(group):
            out[:, pl.ds((k * group + g) * HD, HD)] = res[pl.ds(g * share, share), :].astype(
                out.dtype
            )

    for offset in range(1, n_wide):
        query_copy(offset).wait_send()

    def drain(offset, carry):
        result_copy(offset).wait_send()
        return carry

    lax.fori_loop(1, peers, drain, 0, unroll=peers <= 8)


def local(
    n_wide,
    n_depth,
    patch_store,
    w_key,
    w_value,
    key_gain,
    query_gain,
    queries,
    owner_table,
    reader_table,
    request_image,
    image_tiles,
):
    images, rows, width = patch_store.shape
    kv_local = w_key.shape[1] // HD
    batch, q_cols = queries.shape
    group = q_cols // (kv_local * HD)
    share = batch // n_depth
    block = share * group
    group_rows = n_depth * block
    peers = n_wide * n_depth
    total_rows = peers * block
    anywhere = pl.BlockSpec(memory_space=pl.ANY)
    dma = pltpu.SemaphoreType.DMA
    return pl.pallas_call(
        functools.partial(kernel, n_wide, n_depth),
        out_shape=pltpu.VMEM((share, q_cols), jnp.bfloat16),
        in_specs=[anywhere] * 10,
        out_specs=pl.BlockSpec(memory_space=pltpu.VMEM),
        scratch_shapes=[
            pltpu.SMEM(owner_table.shape, jnp.int32),
            pltpu.SMEM(reader_table.shape, jnp.int32),
            pltpu.SMEM(request_image.shape, jnp.int32),
            pltpu.SMEM(image_tiles.shape, jnp.int32),
            pltpu.VMEM((images, rows, width), jnp.bfloat16),
            pltpu.VMEM((kv_local, width, 2 * HD), jnp.bfloat16),
            pltpu.VMEM((batch, q_cols), jnp.bfloat16),
            pltpu.VMEM((2, 1, HD), jnp.float32),
            pltpu.VMEM((batch, q_cols), jnp.float32),
            pltpu.VMEM((group_rows, HD), jnp.float32),
            pltpu.VMEM((n_wide, kv_local + 1, group_rows, HD), jnp.bfloat16),
            pltpu.VMEM((total_rows, HD), jnp.int32),
            pltpu.VMEM((total_rows, HD), jnp.int32),
            pltpu.VMEM((kv_local, images * rows, 2 * HD), jnp.float32),
            pltpu.VMEM((kv_local, images * rows, HD), jnp.bfloat16),
            pltpu.VMEM((kv_local, images * rows, 2 * HD), jnp.bfloat16),
            pltpu.VMEM((peers, kv_local + 1, block, HD), jnp.bfloat16),
            pltpu.VMEM((peers, kv_local + 1, block, HD), jnp.bfloat16),
            pltpu.VMEM((block, HD), jnp.float32),
            dma((kv_local, CHUNKS, 2)),
            dma((CHUNKS,)),
            dma((7,)),
            dma((n_wide,)),
            dma((n_wide,)),
            dma((peers,)),
            dma((peers,)),
        ],
        compiler_params=pltpu.CompilerParams(
            collective_id=0, has_side_effects=True, vmem_limit_bytes=56 * 1024 * 1024
        ),
    )(
        patch_store,
        w_key,
        w_value,
        key_gain.reshape(1, HD),
        query_gain.reshape(1, HD),
        queries,
        owner_table,
        reader_table,
        request_image,
        image_tiles,
    )


def solution(mesh):
    placed = (
        P("wide", "depth", None),
        P(None, "narrow"),
        P(None, "narrow"),
        P(),
        P(),
        P("wide", "narrow"),
        P(),
        P(),
        P("wide"),
        P(),
    )
    return jax.shard_map(
        functools.partial(local, mesh.shape["wide"], mesh.shape["depth"]),
        mesh=mesh,
        in_specs=placed,
        out_specs=P(("wide", "depth"), "narrow"),
        check_vma=False,
    )
```
